32 devices in a mesh: rows: 4 (over z), width: 4 (over y, x), site: 2 (over core).
Axes of the slice: x: 2, y: 2, z: 4, core: 2. Of those that a mesh axis runs over, the one named last changes fastest.
Arguments:
- weight_query: float32 [8192, 4096], P(('site', 'rows'), 'width'), parts along dimension 0, may hold values from -0.125 to 0.125
- moment_query: float32 [8192, 4096], P(('site', 'rows'), 'width'), parts along dimension 0, may hold values from -6 to 6
- square_query: float32 [8192, 4096], P(('site', 'rows'), 'width'), parts along dimension 0, may hold values from 0.1 to 10
- weight_key: float32 [8192, 1024], P(('site', 'rows'), 'width'), parts along dimension 0, may hold values from -0.125 to 0.125
- moment_key: float32 [8192, 1024], P(('site', 'rows'), 'width'), parts along dimension 0, may hold values from -6 to 6
- square_key: float32 [8192, 1024], P(('site', 'rows'), 'width'), parts along dimension 0, may hold values from 0.1 to 10
- weight_value: float32 [8192, 1024], P(('site', 'rows'), 'width'), parts along dimension 0, may hold values from -0.125 to 0.125
- moment_value: float32 [8192, 1024], P(('site', 'rows'), 'width'), parts along dimension 0, may hold values from -6 to 6
- square_value: float32 [8192, 1024], P(('site', 'rows'), 'width'), parts along dimension 0, may hold values from 0.1 to 10
- norm_train: float32 [8192], P(('site', 'rows', 'width')), parts along dimension 0, may hold values from 0.25 to 1.75
- norm_step: float32 [8192], P(('site', 'rows', 'width')), parts along dimension 0, may hold values from -0.3 to 0.3
Outputs:
- final_query: bfloat16 [8192, 4096], P('site', 'width'), parts along dimension 0
- final_key: bfloat16 [8192, 1024], P('site', 'width'), parts along dimension 0
- final_value: bfloat16 [8192, 1024], P('site', 'width'), parts along dimension 0
- column_query: float32 [8192], P(('site', 'width')), parts along dimension 0
- column_key: float32 [2048], P(('site', 'width')), parts along dimension 0
- column_value: float32 [2048], P(('site', 'width')), parts along dimension 0
- serve_norm: bfloat16 [8192], P('site'), parts along dimension 0
- result_query: float32 [8192, 4096], P(('site', 'rows'), 'width'), parts along dimension 0
- result_key: float32 [8192, 1024], P(('site', 'rows'), 'width'), parts along dimension 0
- result_value: float32 [8192, 1024], P(('site', 'rows'), 'width'), parts along dimension 0
The draws below stay inside these ranges and needn't reach their ends.
There are 2 independent parts, one for each index of `site`. The reference program is written for one: setup_inputs(seed, part) draws one part's arguments, and reference() takes and returns one part's arrays. A program takes and returns all parts, laid end to end along the dimension named above; each array names one. Nothing has to cross between parts.
All inputs are finite; a program needn't handle non-finite values.
Results may differ from the reference program's by a relative error of at most 0.001.
Values may be sent and summed in bfloat16 or wider, within the bound.
A program may use at most 128 MiB of HBM per device.

```python
import math
import jax
import jax.numpy as jnp
from jax import lax

D_MODEL = 4096
Q_DIM = 4096
KV_DIM = 1024


def strengthened(values, rng, source, target, parts, factor):
    def block_of(axis_at):
        return (jnp.arange(values.shape[axis_at]) // (values.shape[axis_at] // parts)).reshape((-1,) + (1,) * (values.ndim - 1 - axis_at))

    near = jax.random.permutation(rng, parts)[block_of(target)]
    far = (block_of(target) + parts // 2) % parts
    return jnp.where((block_of(source) == near) | (block_of(source) == far), factor * values, values)


def shard_levels(rng, shape, split, low, high):
    gain, own = 1.0, jax.random.fold_in(rng, 6)
    for dim, parts in split:
        draws = jnp.exp(jax.random.uniform(jax.random.fold_in(own, dim), (parts,), jnp.float32, low / len(split), high / len(split)))
        gain = gain * jnp.repeat(draws, shape[dim] // parts).reshape([-1 if axis == dim else 1 for axis in range(len(shape))])
    return gain


def bell_draw(key, dims, spread, reach, split=(), kind=jnp.bfloat16):
    loudness = shard_levels(key, dims, split, -0.22, 0.18) if split else 1.0
    result = jax.random.normal(key, dims, jnp.float32) * spread * loudness
    return jnp.minimum(jnp.maximum(result, -reach), reach).astype(kind)


def gaussian_with(rng, dims, width, bound, pieces, heavy, held_as=jnp.bfloat16):
    drawn = width * jax.random.normal(rng, dims, jnp.float32)
    if pieces:
        drawn = drawn * shard_levels(rng, dims, pieces, -0.22, 0.18)
    return jnp.clip(strengthened(drawn, jax.random.fold_in(rng, 3), *heavy), -bound, bound).astype(held_as)


def setup_inputs(seed: int = 0, part: int = 0) -> dict:
    key_of = jax.random.split(jax.random.key(seed), 12)
    own_keys = jax.random.split(jax.random.fold_in(key_of[11], part), 12)
    weight_query = gaussian_with(own_keys[0], (D_MODEL, Q_DIM), D_MODEL ** -0.5, 0.125, ((0, 4), (1, 4)), (0, 1, 4, 2.0), jnp.float32)
    moment_query = bell_draw(own_keys[1], (D_MODEL, Q_DIM), 1.0, 6.0, ((0, 4), (1, 4)), jnp.float32)
    square_query = jnp.clip(jnp.exp(math.log(10.0) - 4.6051702 * jax.random.uniform(own_keys[2], (D_MODEL, Q_DIM), jnp.float32) ** shard_levels(own_keys[2], (D_MODEL, Q_DIM), ((0, 4), (1, 4)), -0.2, 0.2)), 0.1, 10.0)
    weight_key = gaussian_with(own_keys[3], (D_MODEL, KV_DIM), D_MODEL ** -0.5, 0.125, ((0, 4), (1, 4)), (0, 1, 4, 2.0), jnp.float32)
    moment_key = bell_draw(own_keys[4], (D_MODEL, KV_DIM), 1.0, 6.0, ((0, 4), (1, 4)), jnp.float32)
    square_key = jnp.clip(jnp.exp(math.log(10.0) - 4.6051702 * jax.random.uniform(own_keys[5], (D_MODEL, KV_DIM), jnp.float32) ** shard_levels(own_keys[5], (D_MODEL, KV_DIM), ((0, 4), (1, 4)), -0.2, 0.2)), 0.1, 10.0)
    weight_value = gaussian_with(own_keys[6], (D_MODEL, KV_DIM), D_MODEL ** -0.5, 0.125, ((0, 4), (1, 4)), (0, 1, 4, 2.0), jnp.float32)
    moment_value = bell_draw(own_keys[7], (D_MODEL, KV_DIM), 1.0, 6.0, ((0, 4), (1, 4)), jnp.float32)
    square_value = jnp.clip(jnp.exp(math.log(10.0) - 4.6051702 * jax.random.uniform(own_keys[8], (D_MODEL, KV_DIM), jnp.float32) ** shard_levels(own_keys[8], (D_MODEL, KV_DIM), ((0, 4), (1, 4)), -0.2, 0.2)), 0.1, 10.0)
    norm_train = jnp.clip(1.0 + 0.15 * jax.random.normal(own_keys[9], (D_MODEL,), jnp.float32), 0.25, 1.75)
    norm_step = jnp.clip(jax.random.uniform(own_keys[10], (D_MODEL,), jnp.float32, -0.3, 0.3) * shard_levels(own_keys[10], (D_MODEL,), ((0, 16),), -0.4, 0.0), -0.3, 0.3)
    return dict(weight_query=weight_query, moment_query=moment_query, square_query=square_query, weight_key=weight_key, moment_key=moment_key, square_key=square_key, weight_value=weight_value, moment_value=moment_value, square_value=square_value, norm_train=norm_train, norm_step=norm_step)


learn_rate = 0.02
decay_rate = 0.05
tiny_value = 1e-08

def reference(weight_query, moment_query, square_query, weight_key, moment_key, square_key, weight_value, moment_value, square_value, norm_train, norm_step):
    result_query = weight_query - learn_rate * (moment_query / (jnp.sqrt(square_query) + tiny_value) + decay_rate * weight_query)
    result_key = weight_key - learn_rate * (moment_key / (jnp.sqrt(square_key) + tiny_value) + decay_rate * weight_key)
    result_value = weight_value - learn_rate * (moment_value / (jnp.sqrt(square_value) + tiny_value) + decay_rate * weight_value)
    column_query = jnp.sqrt(lax.optimization_barrier(jnp.sum(result_query * result_query, axis=0)))
    final_query = (result_query / column_query).astype(jnp.bfloat16)
    column_key = jnp.sqrt(lax.optimization_barrier(jnp.sum(result_key * result_key, axis=0)))
    final_key = (result_key / column_key).astype(jnp.bfloat16)
    column_value = jnp.sqrt(lax.optimization_barrier(jnp.sum(result_value * result_value, axis=0)))
    final_value = (result_value / column_value).astype(jnp.bfloat16)
    serve_norm = (norm_train + norm_step).astype(jnp.bfloat16)
    return (final_query, final_key, final_value, column_query, column_key, column_value, serve_norm, result_query, result_key, result_value)
```

```python
import functools

import jax
import jax.numpy as jnp
from jax import lax
from jax.experimental import pallas as pl
from jax.experimental.pallas import tpu as pltpu
from jax.sharding import PartitionSpec as P

learn_rate = 0.02
decay_rate = 0.05
tiny_value = 1e-08

LAG = 3
MESH = pl.DeviceIdType.MESH


def chunks_of(widths):
    out = []
    for a, width in enumerate(widths):
        step = 128 if width % 128 == 0 else width
        out += [(a, c, step) for c in range(0, width, step)]
    return out


def kernel(n, wide, chunks, *refs):
    inputs, norm_in = [refs[0:3], refs[3:6], refs[6:9]], refs[9]
    finals, columns, serve, results = refs[10:13], refs[13:16], refs[16], refs[17:20]
    held = [refs[20:23], refs[23:26], refs[26:29]]
    sums, in_sem, sum_send, sum_recv, send, recv, norm_send, norm_recv = refs[29:]
    me, col = lax.axis_index("rows"), lax.axis_index("width")
    flat, group = me * wide + col, n * wide
    depth = results[0].shape[0]
    block = min(depth, 64)

    barrier = pltpu.get_barrier_semaphore()

    def greet(p, carry):
        peer = lax.rem(flat + p, group)
        pl.semaphore_signal(
            barrier, inc=1,
            device_id={"rows": lax.div(peer, wide), "width": lax.rem(peer, wide)},
            device_id_type=MESH,
        )
        return carry

    def load(j, k):
        a, c, cw = chunks[j]
        return pltpu.make_async_copy(
            inputs[a][k].at[:, pl.ds(c, cw)], held[a][k].at[:, pl.ds(c, cw)], in_sem.at[j, k]
        )

    for j in range(len(chunks)):
        for k in range(3):
            load(j, k).start()
    lax.fori_loop(1, group, greet, 0)
    serve[flat] = norm_in[...]

    def update(j):
        a, c, cw = chunks[j]
        for k in range(3):
            load(j, k).wait()
        weight, moment, square = held[a]
        cols = pl.ds(c, cw)

        def body(i, acc):
            rows = pl.ds(pl.multiple_of(i * block, block), block)
            w = weight[rows, cols]
            r = w - learn_rate * (
                moment[rows, cols] / (jnp.sqrt(square[rows, cols]) + tiny_value) + decay_rate * w
            )
            results[a][rows, cols] = r
            return acc + jnp.sum((r * r).reshape(block // 8, 8, cw), axis=0)

        acc = lax.fori_loop(0, depth // block, body, jnp.zeros((8, cw), jnp.float32))
        sums[j, me, :, pl.ds(0, cw)] = jnp.sum(acc, axis=0, keepdims=True)

    def sum_copy(j, p, slot):
        return pltpu.make_async_remote_copy(
            src_ref=sums.at[j, me], dst_ref=sums.at[j, slot],
            send_sem=sum_send.at[j, p], recv_sem=sum_recv.at[j, p],
            device_id={"rows": lax.rem(me + p, n)}, device_id_type=MESH,
        )

    def norm_copy(p, slot):
        peer = lax.rem(flat + p, group)
        return pltpu.make_async_remote_copy(
            src_ref=serve.at[flat], dst_ref=serve.at[slot],
            send_sem=norm_send.at[p], recv_sem=norm_recv.at[p],
            device_id={"rows": lax.div(peer, wide), "width": lax.rem(peer, wide)},
            device_id_type=MESH,
        )

    has_next = (me < n - 1, me > 0)
    step = (1, -1)

    def pass_on(d, h, j, a, cols, origin):
        rows = pl.ds(pl.multiple_of(origin * depth, depth), depth)
        return pltpu.make_async_remote_copy(
            src_ref=finals[a].at[rows, cols], dst_ref=finals[a].at[rows, cols],
            send_sem=send.at[d, h, j], recv_sem=recv.at[d, h, j],
            device_id={"rows": lax.rem(me + step[d] + n, n)}, device_id_type=MESH,
        )

    def finish(j):
        a, c, cw = chunks[j]
        cols = pl.ds(c, cw)
        for p in range(1, n):
            sum_copy(j, p, lax.rem(me - p + n, n)).wait_recv()
        total = sums[j, 0, :, pl.ds(0, cw)]
        for p in range(1, n):
            total = total + sums[j, p, :, pl.ds(0, cw)]
        scale = jnp.sqrt(total)
        columns[a][:, cols] = scale
        inverse = 1.0 / scale

        def body(i, carry):
            rows = pl.ds(pl.multiple_of(i * block, block), block)
            mine = pl.ds(pl.multiple_of(me * depth + i * block, block), block)
            finals[a][mine, cols] = (results[a][rows, cols] * inverse).astype(jnp.bfloat16)
            return carry

        lax.fori_loop(0, depth // block, body, 0)
        for d in (0, 1):
            @pl.when(has_next[d])
            def _(d=d):
                pass_on(d, 0, j, a, cols, me).start()

    for j in range(len(chunks) + LAG):
        if j < len(chunks):
            update(j)
            if j == 0:
                pl.semaphore_wait(barrier, group - 1)
            for p in range(1, n):
                sum_copy(j, p, me).start()
        if j >= LAG:
            finish(j - LAG)

    def send_norm(p, carry):
        norm_copy(p, flat).start()
        return carry

    lax.fori_loop(1, group, send_norm, 0)

    counts = [sum(1 for ch in chunks if ch[0] == a) for a in range(3)]
    bases = [sum(counts[:a]) for a in range(3)]

    def each(visit):
        for h in range(n - 1):
            for a in range(3):
                cw = chunks[bases[a]][2]

                def body(k, carry, h=h, a=a, cw=cw):
                    start = pl.multiple_of(k * cw, 128) if counts[a] > 1 else 0
                    for d in (0, 1):
                        visit(d, h, bases[a] + k, a, pl.ds(start, cw))
                    return carry

                if counts[a] > 1:
                    lax.fori_loop(0, counts[a], body, 0)
                else:
                    body(0, 0)

    def relay(d, h, j, a, cols):
        origin = me - step[d] * (h + 1)

        @pl.when((origin >= 0) & (origin < n))
        def _():
            pass_on(d, h, j, a, cols, origin).wait_recv()

            if h + 1 < n - 1:
                @pl.when(has_next[d])
                def _():
                    pass_on(d, h + 1, j, a, cols, origin).start()

    each(relay)

    def drain(d, h, j, a, cols):
        origin = me - step[d] * h

        @pl.when(has_next[d] & (origin >= 0) & (origin < n))
        def _():
            pass_on(d, h, j, a, cols, origin).wait_send()

    each(drain)
    for j in range(len(chunks)):
        for p in range(1, n):
            sum_copy(j, p, me).wait_send()

    def end_norm(p, carry):
        norm_copy(p, lax.rem(flat - p + group, group)).wait_recv()
        norm_copy(p, flat).wait_send()
        return carry

    lax.fori_loop(1, group, end_norm, 0)


def solution(mesh):
    n, wide = mesh.shape["rows"], mesh.shape["width"]

    def per_device(*args):
        arrays, (norm_train, norm_step) = args[:9], args[9:]
        depth = arrays[0].shape[0]
        widths = [arrays[3 * a].shape[1] for a in range(3)]
        chunks = chunks_of(widths)
        count = len(chunks)
        part = norm_train.shape[0]
        lanes = 128 if part % 128 == 0 else part
        narrow = (norm_train + norm_step).astype(jnp.bfloat16).reshape(part // lanes, lanes)
        group = n * wide
        vmem, dma = pltpu.VMEM, pltpu.SemaphoreType.DMA
        out_shape = (
            [vmem((n * depth, w), jnp.bfloat16) for w in widths]
            + [vmem((1, w), jnp.float32) for w in widths]
            + [vmem((group, part // lanes, lanes), jnp.bfloat16)]
            + [vmem((depth, w), jnp.float32) for w in widths]
        )
        padded = sum(-(-w // 128) * 128 for w in widths)
        outside = padded * depth * (2 * n + 4) + (1 << 20)
        outs = pl.pallas_call(
            functools.partial(kernel, n, wide, chunks),
            out_shape=out_shape,
            in_specs=[pl.BlockSpec(memory_space=pltpu.HBM)] * 9 + [pl.BlockSpec(memory_space=vmem)],
            out_specs=[pl.BlockSpec(memory_space=vmem)] * 10,
            scratch_shapes=[vmem((depth, w), jnp.float32) for w in widths for _ in range(3)]
            + [
                vmem((count, n, 1, 128), jnp.float32),
                dma((count, 3)),
                dma((count, n)),
                dma((count, n)),
                dma((2, n - 1, count)),
                dma((2, n - 1, count)),
                dma((group,)),
                dma((group,)),
            ],
            compiler_params=pltpu.CompilerParams(
                collective_id=0,
                has_side_effects=True,
                vmem_limit_bytes=60 * (1 << 20) - outside,
            ),
        )(*arrays, narrow)
        return (
            *outs[0:3],
            *(c.reshape(-1) for c in outs[3:6]),
            outs[6].reshape(-1),
            *outs[7:10],
        )

    cut = P(("site", "rows"), "width")
    return jax.shard_map(
        per_device,
        mesh=mesh,
        in_specs=(cut,) * 9 + (P(("site", "rows", "width")),) * 2,
        out_specs=(P("site", "width"),) * 3
        + (P(("site", "width")),) * 3
        + (P("site"),)
        + (cut,) * 3,
        check_vma=False,
    )
```

```python
import functools

import jax
import jax.numpy as jnp
from jax import lax
from jax.experimental import pallas as pl
from jax.experimental.pallas import tpu as pltpu
from jax.sharding import PartitionSpec as P

learn_rate = 0.02
decay_rate = 0.05
tiny_value = 1e-08

LAG = 3
MESH = pl.DeviceIdType.MESH


def chunks_of(widths):
    out = []
    for a, width in enumerate(widths):
        step = 128 if width % 128 == 0 else width
        out += [(a, c, step) for c in range(0, width, step)]
    return out


def kernel(n, wide, chunks, *refs):
    inputs, norms = [refs[0:3], refs[3:6], refs[6:9]], refs[9:11]
    finals, columns, serve, results = refs[11:14], refs[14:17], refs[17], refs[18:21]
    held = [refs[21:24], refs[24:27], refs[27:30]]
    gain, sums, in_sem, gain_sem, sum_send, sum_recv, send, recv, norm_send, norm_recv = refs[30:]
    me, col = lax.axis_index("rows"), lax.axis_index("width")
    flat, group = me * wide + col, n * wide
    depth = results[0].shape[0]
    block = min(depth, 64)

    barrier = pltpu.get_barrier_semaphore()

    def greet(p, carry):
        peer = lax.rem(flat + p, group)
        pl.semaphore_signal(
            barrier, inc=1,
            device_id={"rows": lax.div(peer, wide), "width": lax.rem(peer, wide)},
            device_id_type=MESH,
        )
        return carry

    def load(j, k):
        a, c, cw = chunks[j]
        return pltpu.make_async_copy(
            inputs[a][k].at[:, pl.ds(c, cw)], held[a][k].at[:, pl.ds(c, cw)], in_sem.at[j, k]
        )

    for j in range(len(chunks)):
        for k in range(3):
            load(j, k).start()
    for k in range(2):
        pltpu.make_async_copy(norms[k], gain.at[k], gain_sem.at[k]).start()
    lax.fori_loop(1, group, greet, 0)

    def update(j):
        a, c, cw = chunks[j]
        for k in range(3):
            load(j, k).wait()
        weight, moment, square = held[a]
        cols = pl.ds(c, cw)

        def body(i, acc):
            rows = pl.ds(pl.multiple_of(i * block, block), block)
            w = weight[rows, cols]
            r = w - learn_rate * (
                moment[rows, cols] / (jnp.sqrt(square[rows, cols]) + tiny_value) + decay_rate * w
            )
            results[a][rows, cols] = r
            return acc + jnp.sum((r * r).reshape(block // 8, 8, cw), axis=0)

        acc = lax.fori_loop(0, depth // block, body, jnp.zeros((8, cw), jnp.float32))
        sums[j, me, :, pl.ds(0, cw)] = jnp.sum(acc, axis=0, keepdims=True)

    def sum_copy(j, p, slot):
        return pltpu.make_async_remote_copy(
            src_ref=sums.at[j, me], dst_ref=sums.at[j, slot],
            send_sem=sum_send.at[j, p], recv_sem=sum_recv.at[j, p],
            device_id={"rows": lax.rem(me + p, n)}, device_id_type=MESH,
        )

    def norm_copy(p, slot):
        peer = lax.rem(flat + p, group)
        return pltpu.make_async_remote_copy(
            src_ref=serve.at[flat], dst_ref=serve.at[slot],
            send_sem=norm_send.at[p], recv_sem=norm_recv.at[p],
            device_id={"rows": lax.div(peer, wide), "width": lax.rem(peer, wide)},
            device_id_type=MESH,
        )

    has_next = (me < n - 1, me > 0)
    step = (1, -1)

    def pass_on(d, h, j, a, cols, origin):
        rows = pl.ds(pl.multiple_of(origin * depth, depth), depth)
        return pltpu.make_async_remote_copy(
            src_ref=finals[a].at[rows, cols], dst_ref=finals[a].at[rows, cols],
            send_sem=send.at[d, h, j], recv_sem=recv.at[d, h, j],
            device_id={"rows": lax.rem(me + step[d] + n, n)}, device_id_type=MESH,
        )

    def finish(j):
        a, c, cw = chunks[j]
        cols = pl.ds(c, cw)
        for p in range(1, n):
            sum_copy(j, p, lax.rem(me - p + n, n)).wait_recv()
        total = sums[j, 0, :, pl.ds(0, cw)]
        for p in range(1, n):
            total = total + sums[j, p, :, pl.ds(0, cw)]
        scale = jnp.sqrt(total)
        columns[a][:, cols] = scale
        inverse = 1.0 / scale

        def body(i, carry):
            rows = pl.ds(pl.multiple_of(i * block, block), block)
            mine = pl.ds(pl.multiple_of(me * depth + i * block, block), block)
            finals[a][mine, cols] = (results[a][rows, cols] * inverse).astype(jnp.bfloat16)
            return carry

        lax.fori_loop(0, depth // block, body, 0)
        for d in (0, 1):
            @pl.when(has_next[d])
            def _(d=d):
                pass_on(d, 0, j, a, cols, me).start()

    for j in range(len(chunks) + LAG):
        if j < len(chunks):
            update(j)
            if j == 0:
                pl.semaphore_wait(barrier, group - 1)
            for p in range(1, n):
                sum_copy(j, p, me).start()
        if j >= LAG:
            finish(j - LAG)

    for k in range(2):
        pltpu.make_async_copy(norms[k], gain.at[k], gain_sem.at[k]).wait()
    serve[flat] = (gain[0] + gain[1]).astype(jnp.bfloat16)

    def send_norm(p, carry):
        norm_copy(p, flat).start()
        return carry

    lax.fori_loop(1, group, send_norm, 0)

    counts = [sum(1 for ch in chunks if ch[0] == a) for a in range(3)]
    bases = [sum(counts[:a]) for a in range(3)]

    def each(visit):
        for h in range(n - 1):
            for a in range(3):
                cw = chunks[bases[a]][2]

                def body(k, carry, h=h, a=a, cw=cw):
                    start = pl.multiple_of(k * cw, 128) if counts[a] > 1 else 0
                    for d in (0, 1):
                        visit(d, h, bases[a] + k, a, pl.ds(start, cw))
                    return carry

                if counts[a] > 1:
                    lax.fori_loop(0, counts[a], body, 0)
                else:
                    body(0, 0)

    def relay(d, h, j, a, cols):
        origin = me - step[d] * (h + 1)

        @pl.when((origin >= 0) & (origin < n))
        def _():
            pass_on(d, h, j, a, cols, origin).wait_recv()

            if h + 1 < n - 1:
                @pl.when(has_next[d])
                def _():
                    pass_on(d, h + 1, j, a, cols, origin).start()

    each(relay)

    def drain(d, h, j, a, cols):
        origin = me - step[d] * h

        @pl.when(has_next[d] & (origin >= 0) & (origin < n))
        def _():
            pass_on(d, h, j, a, cols, origin).wait_send()

    each(drain)
    for j in range(len(chunks)):
        for p in range(1, n):
            sum_copy(j, p, me).wait_send()

    def end_norm(p, carry):
        norm_copy(p, lax.rem(flat - p + group, group)).wait_recv()
        norm_copy(p, flat).wait_send()
        return carry

    lax.fori_loop(1, group, end_norm, 0)


def store(pieces, *refs):
    count = len(pieces)
    sem = refs[2 * count]
    copies = []
    for k, cut in enumerate(pieces):
        rows = refs[k].shape[0] // cut
        for i in range(cut):
            part = pl.ds(i * rows, rows)
            copies.append(
                pltpu.make_async_copy(
                    refs[k].at[part], refs[count + k].at[part], sem.at[len(copies)]
                )
            )
    for copy in copies:
        copy.start()
    for copy in copies:
        copy.wait()


def solution(mesh):
    n, wide = mesh.shape["rows"], mesh.shape["width"]

    def per_device(*args):
        arrays, (norm_train, norm_step) = args[:9], args[9:]
        depth = arrays[0].shape[0]
        widths = [arrays[3 * a].shape[1] for a in range(3)]
        chunks = chunks_of(widths)
        count = len(chunks)
        part = norm_train.shape[0]
        lanes = 128 if part % 128 == 0 else part
        norms = [x.reshape(part // lanes, lanes) for x in (norm_train, norm_step)]
        group = n * wide
        vmem, dma = pltpu.VMEM, pltpu.SemaphoreType.DMA
        out_shape = (
            [vmem((n * depth, w), jnp.bfloat16) for w in widths]
            + [vmem((1, w), jnp.float32) for w in widths]
            + [vmem((group, part // lanes, lanes), jnp.bfloat16)]
            + [vmem((depth, w), jnp.float32) for w in widths]
        )
        padded = sum(-(-w // 128) * 128 for w in widths)
        outside = padded * depth * (2 * n + 4) + (1 << 20)
        outs = pl.pallas_call(
            functools.partial(kernel, n, wide, chunks),
            out_shape=out_shape,
            in_specs=[pl.BlockSpec(memory_space=pltpu.HBM)] * 11,
            out_specs=[pl.BlockSpec(memory_space=vmem)] * 10,
            scratch_shapes=[vmem((depth, w), jnp.float32) for w in widths for _ in range(3)]
            + [
                vmem((2, part // lanes, lanes), jnp.float32),
                vmem((count, n, 1, 128), jnp.float32),
                dma((count, 3)),
                dma((2,)),
                dma((count, n)),
                dma((count, n)),
                dma((2, n - 1, count)),
                dma((2, n - 1, count)),
                dma((group,)),
                dma((group,)),
            ],
            compiler_params=pltpu.CompilerParams(
                collective_id=0,
                has_side_effects=True,
                vmem_limit_bytes=60 * (1 << 20) - outside,
            ),
        )(*arrays, *norms)
        pieces = [n, 1, 1, 1, 1, 1, 1, 2, 1, 1]
        outs = pl.pallas_call(
            functools.partial(store, pieces),
            out_shape=[jax.ShapeDtypeStruct(x.shape, x.dtype) for x in outs],
            in_specs=[pl.BlockSpec(memory_space=vmem)] * 10,
            out_specs=[pl.BlockSpec(memory_space=pltpu.HBM)] * 10,
            scratch_shapes=[dma((sum(pieces),))],
            compiler_params=pltpu.CompilerParams(vmem_limit_bytes=1 << 20),
        )(*(pltpu.with_memory_space_constraint(x, vmem) for x in outs))
        return (
            *outs[0:3],
            *(c.reshape(-1) for c in outs[3:6]),
            outs[6].reshape(-1),
            *outs[7:10],
        )

    cut = P(("site", "rows"), "width")
    return jax.shard_map(
        per_device,
        mesh=mesh,
        in_specs=(cut,) * 9 + (P(("site", "rows", "width")),) * 2,
        out_specs=(P("site", "width"),) * 3
        + (P(("site", "width")),) * 3
        + (P("site"),)
        + (cut,) * 3,
        check_vma=False,
    )
```

```python
import functools

import jax
import jax.numpy as jnp
from jax import lax
from jax.experimental import pallas as pl
from jax.experimental.pallas import tpu as pltpu
from jax.sharding import PartitionSpec as P

learn_rate = 0.02
decay_rate = 0.05
tiny_value = 1e-08

LAG = 1
MESH = pl.DeviceIdType.MESH


def chunks_of(widths):
    out = []
    for a, width in enumerate(widths):
        step = 128 if width % 128 == 0 else width
        out += [(a, c, step) for c in range(0, width, step)]
    return out


def kernel(n, wide, chunks, *refs):
    inputs, norms = [refs[0:3], refs[3:6], refs[6:9]], refs[9:11]
    finals, columns, serve, results = refs[11:14], refs[14:17], refs[17], refs[18:21]
    held = [refs[21:24], refs[24:27], refs[27:30]]
    gain, sums, in_sem, gain_sem, sum_send, sum_recv, send, recv, norm_send, norm_recv = refs[30:]
    me, col = lax.axis_index("rows"), lax.axis_index("width")
    flat, group = me * wide + col, n * wide
    depth = results[0].shape[0]
    block = min(depth, 64)

    barrier = pltpu.get_barrier_semaphore()

    def greet(p, carry):
        peer = lax.rem(flat + p, group)
        pl.semaphore_signal(
            barrier, inc=1,
            device_id={"rows": lax.div(peer, wide), "width": lax.rem(peer, wide)},
            device_id_type=MESH,
        )
        return carry

    def load(j, k):
        a, c, cw = chunks[j]
        return pltpu.make_async_copy(
            inputs[a][k].at[:, pl.ds(c, cw)], held[a][k].at[:, pl.ds(c, cw)], in_sem.at[j, k]
        )

    ahead = min(2, len(chunks))
    for j in range(ahead):
        for k in range(3):
            load(j, k).start()
    for k in range(2):
        pltpu.make_async_copy(norms[k], gain.at[k], gain_sem.at[k]).start()
    lax.fori_loop(1, group, greet, 0)

    def update(j):
        a, c, cw = chunks[j]
        for k in range(3):
            load(j, k).wait()
        if j + ahead < len(chunks):
            for k in range(3):
                load(j + ahead, k).start()
        weight, moment, square = held[a]
        cols = pl.ds(c, cw)

        def body(i, acc):
            rows = pl.ds(pl.multiple_of(i * block, block), block)
            w = weight[rows, cols]
            r = w - learn_rate * (
                moment[rows, cols] / (jnp.sqrt(square[rows, cols]) + tiny_value) + decay_rate * w
            )
            results[a][rows, cols] = r
            return acc + jnp.sum((r * r).reshape(block // 8, 8, cw), axis=0)

        acc = lax.fori_loop(0, depth // block, body, jnp.zeros((8, cw), jnp.float32))
        sums[j, me, :, pl.ds(0, cw)] = jnp.sum(acc, axis=0, keepdims=True)

    def sum_copy(j, p, slot):
        return pltpu.make_async_remote_copy(
            src_ref=sums.at[j, me], dst_ref=sums.at[j, slot],
            send_sem=sum_send.at[j, p], recv_sem=sum_recv.at[j, p],
            device_id={"rows": lax.rem(me + p, n)}, device_id_type=MESH,
        )

    def norm_copy(p, slot):
        peer = lax.rem(flat + p, group)
        return pltpu.make_async_remote_copy(
            src_ref=serve.at[flat], dst_ref=serve.at[slot],
            send_sem=norm_send.at[p], recv_sem=norm_recv.at[p],
            device_id={"rows": lax.div(peer, wide), "width": lax.rem(peer, wide)},
            device_id_type=MESH,
        )

    has_next = (me < n - 1, me > 0)
    step = (1, -1)

    def pass_on(d, h, j, a, cols, origin):
        rows = pl.ds(pl.multiple_of(origin * depth, depth), depth)
        return pltpu.make_async_remote_copy(
            src_ref=finals[a].at[rows, cols], dst_ref=finals[a].at[rows, cols],
            send_sem=send.at[d, h, j], recv_sem=recv.at[d, h, j],
            device_id={"rows": lax.rem(me + step[d] + n, n)}, device_id_type=MESH,
        )

    def finish(j):
        a, c, cw = chunks[j]
        cols = pl.ds(c, cw)
        for p in range(1, n):
            sum_copy(j, p, lax.rem(me - p + n, n)).wait_recv()
        total = sums[j, 0, :, pl.ds(0, cw)]
        for p in range(1, n):
            total = total + sums[j, p, :, pl.ds(0, cw)]
        scale = jnp.sqrt(total)
        columns[a][:, cols] = scale
        inverse = 1.0 / scale

        def body(i, carry):
            rows = pl.ds(pl.multiple_of(i * block, block), block)
            mine = pl.ds(pl.multiple_of(me * depth + i * block, block), block)
            finals[a][mine, cols] = (results[a][rows, cols] * inverse).astype(jnp.bfloat16)
            return carry

        lax.fori_loop(0, depth // block, body, 0)
        for d in (0, 1):
            @pl.when(has_next[d])
            def _(d=d):
                pass_on(d, 0, j, a, cols, me).start()

    for j in range(len(chunks) + LAG):
        if j < len(chunks):
            update(j)
            if j == 0:
                pl.semaphore_wait(barrier, group - 1)
            for p in range(1, n):
                sum_copy(j, p, me).start()
        if j >= LAG:
            finish(j - LAG)

    for k in range(2):
        pltpu.make_async_copy(norms[k], gain.at[k], gain_sem.at[k]).wait()
    serve[flat] = (gain[0] + gain[1]).astype(jnp.bfloat16)

    def send_norm(p, carry):
        norm_copy(p, flat).start()
        return carry

    lax.fori_loop(1, group, send_norm, 0)

    counts = [sum(1 for ch in chunks if ch[0] == a) for a in range(3)]
    bases = [sum(counts[:a]) for a in range(3)]

    def each(visit):
        for h in range(n - 1):
            for a in range(3):
                cw = chunks[bases[a]][2]

                def body(k, carry, h=h, a=a, cw=cw):
                    start = pl.multiple_of(k * cw, 128) if counts[a] > 1 else 0
                    for d in (0, 1):
                        visit(d, h, bases[a] + k, a, pl.ds(start, cw))
                    return carry

                if counts[a] > 1:
                    lax.fori_loop(0, counts[a], body, 0)
                else:
                    body(0, 0)

    def relay(d, h, j, a, cols):
        origin = me - step[d] * (h + 1)

        @pl.when((origin >= 0) & (origin < n))
        def _():
            pass_on(d, h, j, a, cols, origin).wait_recv()

            if h + 1 < n - 1:
                @pl.when(has_next[d])
                def _():
                    pass_on(d, h + 1, j, a, cols, origin).start()

    each(relay)

    def drain(d, h, j, a, cols):
        origin = me - step[d] * h

        @pl.when(has_next[d] & (origin >= 0) & (origin < n))
        def _():
            pass_on(d, h, j, a, cols, origin).wait_send()

    each(drain)
    for j in range(len(chunks)):
        for p in range(1, n):
            sum_copy(j, p, me).wait_send()

    def end_norm(p, carry):
        norm_copy(p, lax.rem(flat - p + group, group)).wait_recv()
        norm_copy(p, flat).wait_send()
        return carry

    lax.fori_loop(1, group, end_norm, 0)


def store(pieces, *refs):
    count = len(pieces)
    sem = refs[2 * count]
    copies = []
    for k, cut in enumerate(pieces):
        rows = refs[k].shape[0] // cut
        for i in range(cut):
            part = pl.ds(i * rows, rows)
            copies.append(
                pltpu.make_async_copy(
                    refs[k].at[part], refs[count + k].at[part], sem.at[len(copies)]
                )
            )
    for copy in copies:
        copy.start()
    for copy in copies:
        copy.wait()


def solution(mesh):
    n, wide = mesh.shape["rows"], mesh.shape["width"]

    def per_device(*args):
        arrays, (norm_train, norm_step) = args[:9], args[9:]
        depth = arrays[0].shape[0]
        widths = [arrays[3 * a].shape[1] for a in range(3)]
        chunks = chunks_of(widths)
        count = len(chunks)
        part = norm_train.shape[0]
        lanes = 128 if part % 128 == 0 else part
        norms = [x.reshape(part // lanes, lanes) for x in (norm_train, norm_step)]
        group = n * wide
        vmem, dma = pltpu.VMEM, pltpu.SemaphoreType.DMA
        out_shape = (
            [vmem((n * depth, w), jnp.bfloat16) for w in widths]
            + [vmem((1, w), jnp.float32) for w in widths]
            + [vmem((group, part // lanes, lanes), jnp.bfloat16)]
            + [vmem((depth, w), jnp.float32) for w in widths]
        )
        padded = sum(-(-w // 128) * 128 for w in widths)
        outside = padded * depth * (2 * n + 4) + (1 << 20)
        outs = pl.pallas_call(
            functools.partial(kernel, n, wide, chunks),
            out_shape=out_shape,
            in_specs=[pl.BlockSpec(memory_space=pltpu.HBM)] * 11,
            out_specs=[pl.BlockSpec(memory_space=vmem)] * 10,
            scratch_shapes=[vmem((depth, w), jnp.float32) for w in widths for _ in range(3)]
            + [
                vmem((2, part // lanes, lanes), jnp.float32),
                vmem((count, n, 1, 128), jnp.float32),
                dma((count, 3)),
                dma((2,)),
                dma((count, n)),
                dma((count, n)),
                dma((2, n - 1, count)),
                dma((2, n - 1, count)),
                dma((group,)),
                dma((group,)),
            ],
            compiler_params=pltpu.CompilerParams(
                collective_id=0,
                has_side_effects=True,
                vmem_limit_bytes=60 * (1 << 20) - outside,
            ),
        )(*arrays, *norms)
        pieces = [n, 1, 1, 1, 1, 1, 1, 2, 1, 1]
        outs = pl.pallas_call(
            functools.partial(store, pieces),
            out_shape=[jax.ShapeDtypeStruct(x.shape, x.dtype) for x in outs],
            in_specs=[pl.BlockSpec(memory_space=vmem)] * 10,
            out_specs=[pl.BlockSpec(memory_space=pltpu.HBM)] * 10,
            scratch_shapes=[dma((sum(pieces),))],
            compiler_params=pltpu.CompilerParams(vmem_limit_bytes=1 << 20),
        )(*(pltpu.with_memory_space_constraint(x, vmem) for x in outs))
        return (
            *outs[0:3],
            *(c.reshape(-1) for c in outs[3:6]),
            outs[6].reshape(-1),
            *outs[7:10],
        )

    cut = P(("site", "rows"), "width")
    return jax.shard_map(
        per_device,
        mesh=mesh,
        in_specs=(cut,) * 9 + (P(("site", "rows", "width")),) * 2,
        out_specs=(P("site", "width"),) * 3
        + (P(("site", "width")),) * 3
        + (P("site"),)
        + (cut,) * 3,
        check_vma=False,
    )
```
